256 devices in a mesh: row: 8 (over x, core), col: 32 (over y, z).
Axes of the slice: x: 4, y: 4, z: 8, core: 2. Of those that a mesh axis runs over, the one named last changes fastest.
Arguments:
- matrix: float32 [2048, 65536], P('col', 'row'), may hold values from -6 to 6
- basis: float32 [65536, 512], P(('row', 'col')), may hold values from -0.0234375 to 0.0234375
Outputs:
- root: float32 [512, 512], P('row', 'col')
- right: float32 [2048, 512], P('col')
The draws below stay inside these ranges and needn't reach their ends.
All inputs are finite; a program needn't handle non-finite values.
Results may differ from the reference program's by a relative error of at most 0.00018.
Values sent between devices are 32-bit elements; how exact they have to be, the bound alone decides.
No kernel may reach another device: no remote copies, remote signals or barrier semaphores. Data moves between devices by JAX's collectives and lax.ppermute only.
A program may use at most 64 MiB of HBM per device.

```python
import jax
import jax.numpy as jnp
from jax import lax

N = 2048
K = 512
ITERS = 8
M = 65536


def steps_of(own_key, extent, split, smallest, largest):
    def one(axis_at, shards_of):
        draws = jax.random.uniform(jax.random.fold_in(jax.random.fold_in(own_key, 6), axis_at), (shards_of,), jnp.float32, smallest / len(split), largest / len(split))
        return jnp.repeat(jnp.exp(draws), extent[axis_at] // shards_of).reshape((-1,) + (1,) * (len(extent) - axis_at - 1))

    gain = one(*split[0])
    for cut in split[1:]:
        gain = gain * one(*cut)
    return gain


def noise(stream_key, dims, width, bound, cuts=(), kind=jnp.bfloat16):
    level = steps_of(stream_key, dims, cuts, -0.22, 0.18) if cuts else 1.0
    drawn = jax.random.normal(stream_key, dims, jnp.float32) * width * level
    return jnp.minimum(jnp.maximum(drawn, -bound), bound).astype(kind)


def setup_inputs(seed: int = 0) -> dict:
    seeds = jax.random.split(jax.random.key(seed), 3)
    matrix = noise(seeds[0], (N, M), 1.0, 6.0, ((0, 32), (1, 8)), jnp.float32)
    basis = noise(seeds[1], (M, K), M ** -0.5, 0.0234375, ((0, 256),), jnp.float32)
    return dict(matrix=matrix, basis=basis)


def reference(matrix, basis):
    highest = lax.Precision.HIGHEST
    proj = lax.dot_general(basis, matrix, (((0,), (1,)), ((), ())), precision=highest)
    gram = jnp.dot(proj, proj.T, precision=highest)
    scale = jnp.sqrt(jnp.sum(gram * gram) + 1e-06)
    ident = jnp.eye(K, dtype=jnp.float32)
    upper = gram / scale
    lower = ident
    for step in range(ITERS):
        middle = 0.5 * (3.0 * ident - jnp.dot(lower, upper, precision=highest))
        upper = jnp.dot(upper, middle, precision=highest)
        lower = jnp.dot(middle, lower, precision=highest)
    root_scale = jnp.sqrt(scale)
    root = upper * root_scale
    right = jnp.dot(proj.T, lower, precision=highest) / root_scale
    return (root, right)
```

```python
import functools

import jax
import jax.numpy as jnp
from jax import lax
from jax.experimental import pallas as pl
from jax.experimental.pallas import tpu as pltpu
from jax.sharding import Mesh
from jax.sharding import PartitionSpec as P

ITERS = 8
HIGHEST = lax.Precision.HIGHEST


def shift(value, axis, by):
    size = lax.axis_size(axis)
    return lax.ppermute(value, axis, [(i, (i + by) % size) for i in range(size)])


def high_low(value):
    high = value.astype(jnp.bfloat16)
    return high, (value - high.astype(jnp.float32)).astype(jnp.bfloat16)


def dot3(left, right):
    (lh, ll), (rh, rl) = left, right
    dot = functools.partial(jnp.dot, preferred_element_type=jnp.float32)
    return dot(lh, rh) + (dot(lh, rl) + dot(ll, rh))


WHOLE = pl.BlockSpec(memory_space=pltpu.VMEM)
SCALARS = pl.BlockSpec(memory_space=pltpu.SMEM)


def column(where, offset, depth, count):
    return pl.multiple_of(lax.rem(where + (offset + count), count) * depth, depth)


def first_kernel(offsets, nz, at, q0, q1, q2, q3, own, *rest):
    pieces, (acc, high, low) = rest[:-3], rest[-3:]
    lines = q0.shape[0]
    for k, quarter in enumerate((q0, q1, q2, q3)):
        rows = pl.ds(pl.multiple_of(lax.rem(at[0] + k, 4) * lines, lines), lines)
        high[rows, :], low[rows, :] = high_low(quarter[...])
    depth = own.shape[0]
    cols = pl.ds(column(at[1], 0, depth, nz), depth)
    acc[...] = dot3((high[:, cols], low[:, cols]), high_low(own[...]))
    add_chunks(offsets, nz, at, high, low, pieces, acc)


def add_chunks(offsets, nz, at, high, low, pieces, acc):
    for i, offset in enumerate(offsets):
        chunk = jnp.concatenate([pieces[2 * i][...], pieces[2 * i + 1][...]], axis=0)
        depth = chunk.shape[0]
        cols = pl.ds(column(at[1], offset, depth, nz), depth)
        acc[...] += dot3((high[:, cols], low[:, cols]), high_low(chunk))


def middle_kernel(offsets, nz, at, high, low, before, *rest):
    pieces, acc = rest[:-1], rest[-1]
    acc[...] = before[...]
    add_chunks(offsets, nz, at, high, low, pieces, acc)


def last_kernel(offsets, nz, share, at, high, low, before, *rest):
    pieces, (keep, give, acc) = rest[:-3], rest[-3:]
    acc[...] = before[...]
    add_chunks(offsets, nz, at, high, low, pieces, acc)
    for i in range(keep.shape[0] // share):
        for core, out in ((at[2], keep), (1 - at[2], give)):
            rows = pl.ds(pl.multiple_of((2 * i + core) * share, share), share)
            out[i * share : (i + 1) * share, :] = acc[rows, :]


def cost(flops, size):
    return pl.CostEstimate(flops=flops, bytes_accessed=size, transcendentals=0)


def f32(*shape):
    return jax.ShapeDtypeStruct(shape, jnp.float32)


def bf16(*shape):
    return jax.ShapeDtypeStruct(shape, jnp.bfloat16)


def polar_kernel(row_ref, gram_ref, proj_ref, root_ref, right_ref, mh, ml, mf, xf):
    width = gram_ref.shape[0]
    height, lines = root_ref.shape[0], proj_ref.shape[0]
    gram = gram_ref[...]
    scale = jnp.sqrt(jnp.sum(gram * gram) + 1e-06)
    root_scale = jnp.sqrt(scale)
    upper = gram / scale
    mf[...] = upper
    mh[...], ml[...] = high_low(upper)
    mine = mf[pl.ds(pl.multiple_of(row_ref[0] * height, height), height), :]
    xf[:height, :] = mine
    xf[height:, :] = proj_ref[...]

    def advance():
        x = xf[...]
        xf[...] = 1.5 * x - 0.5 * dot3(high_low(x), (mh[...], ml[...]))

    def step(_, carry):
        m = (mh[...], ml[...])
        part = 1.5 * mf[...] - 0.5 * dot3(m, m)
        advance()
        new = 1.5 * part - 0.5 * dot3(high_low(part), m)
        mf[...] = new
        mh[...], ml[...] = high_low(new)
        return carry

    lax.fori_loop(0, ITERS - 1, step, 0)
    advance()
    root_ref[...] = xf[:height, :] * root_scale
    right_ref[...] = xf[height:, :] / root_scale


def polar(row, gram, proj, height):
    width = gram.shape[0]
    half = pltpu.VMEM((width, width), jnp.bfloat16)
    return pl.pallas_call(
        polar_kernel,
        out_shape=(f32(height, width), f32(*proj.shape)),
        in_specs=[SCALARS, WHOLE, WHOLE],
        out_specs=(WHOLE, WHOLE),
        scratch_shapes=[
            half,
            half,
            pltpu.VMEM((width, width), jnp.float32),
            pltpu.VMEM((height + proj.shape[0], width), jnp.float32),
        ],
        name="polar",
    )(row, gram, proj)


def local(matrix, basis):
    width = basis.shape[1]
    nx, nc, ny, nz = (lax.axis_size(a) for a in ("x", "core", "y", "z"))
    x, c, y, z = (lax.axis_index(a) for a in ("x", "core", "y", "z"))
    depth = basis.shape[0]
    nrow, ncol = nx * nc, ny * nz
    lines = matrix.shape[0]

    span = depth * nz

    def part(k):
        return lax.dynamic_slice(matrix, (0, lax.rem(y + k, ny) * span), (lines, span))

    half = depth // 2
    chunks = {}
    fwd = [basis[:half], basis[half:]]
    bwd = list(fwd)
    quarters = [part(0), None, None, None]
    for k in range(1, nz // 2 + 1):
        for piece in range(2):
            if k < nz // 2 or piece == 0:
                fwd[piece] = shift(fwd[piece], "z", 1)
            if k < nz // 2 or piece == 1:
                bwd[piece] = shift(bwd[piece], "z", -1)
        if k < nz // 2:
            chunks[-k], chunks[k] = tuple(fwd), tuple(bwd)
        else:
            chunks[k] = (fwd[0], bwd[1])
        if k < ny:
            quarters[-k % ny] = shift(part(k), "y", k)

    at = jnp.stack([y, z, c]).astype(jnp.int32)
    high = bf16(ny * lines, span)
    total = f32(ny * lines, width)
    each = 6 * ny * lines * depth * width

    def pieces_of(offsets):
        return [piece for k in offsets for piece in chunks[k]]

    offsets = (1, -1, 2, -2)
    acc, high, low = pl.pallas_call(
        functools.partial(first_kernel, offsets, nz),
        out_shape=(total, high, high),
        in_specs=[SCALARS] + [WHOLE] * (5 + 2 * len(offsets)),
        out_specs=(WHOLE,) * 3,
        cost_estimate=cost(5 * each, 8 << 20),
        name="first_chunks",
    )(at, *quarters, basis, *pieces_of(offsets))
    offsets = (3, -3)
    acc = pl.pallas_call(
        functools.partial(middle_kernel, offsets, nz),
        out_shape=total,
        in_specs=[SCALARS] + [WHOLE] * (3 + 2 * len(offsets)),
        out_specs=WHOLE,
        cost_estimate=cost(2 * each, 4 << 20),
        name="middle_chunks",
    )(at, high, low, acc, *pieces_of(offsets))
    offsets = (4,)
    share = lines // nrow
    keep, give = pl.pallas_call(
        functools.partial(last_kernel, offsets, nz, share),
        out_shape=(f32(ny * lines // nc, width),) * 2,
        in_specs=[SCALARS] + [WHOLE] * (3 + 2 * len(offsets)),
        out_specs=(WHOLE,) * 2,
        scratch_shapes=[pltpu.VMEM((ny * lines, width), jnp.float32)],
        cost_estimate=cost(each, 3 << 20),
        name="last_chunk",
    )(at, high, low, acc, *pieces_of(offsets))
    total = (keep + shift(give, "core", 1)).reshape(ny * nx, share, width)
    tiles = lax.all_to_all(total, ("y", "x"), 0, 0, tiled=True)
    own = tiles.sum(axis=0)
    copies = jnp.broadcast_to(own, (ny * nx, share, width))
    mine = lax.all_to_all(copies, ("y", "x"), 0, 0, tiled=True)
    other = shift(mine, "core", 1)
    even = jnp.where(c == 0, mine, other)
    odd = jnp.where(c == 0, other, mine)
    proj = jnp.stack([even, odd], axis=1).reshape(ny * lines, width)
    here = lax.dynamic_slice(proj, (y * lines, 0), (lines, width))
    tall = width // (ny * nrow)
    index = (y * nx + x) * nc + c
    some = lax.dynamic_slice(proj, (0, index * tall), (ny * lines, tall))
    gram = lax.dot_general(some, proj, (((0,), (0,)), ((), ())), precision=HIGHEST)
    copies = jnp.broadcast_to(gram, (nz, tall, width))
    gram = lax.all_to_all(copies, "z", 0, 0, tiled=True).sum(axis=0)
    copies = jnp.broadcast_to(gram, (ny * nx, tall, width))
    gram = lax.all_to_all(copies, ("y", "x"), 0, 0, tiled=True)
    other = shift(gram, "core", 1)
    even = jnp.where(c == 0, gram, other)
    odd = jnp.where(c == 0, other, gram)
    gram = jnp.stack([even, odd], axis=1).reshape(width, width)
    row = x * nc + c
    root, right = polar(row.reshape(1), gram, here, width // nrow)
    root = lax.dynamic_slice(root, (0, (y * nz + z) * (width // ncol)), (width // nrow, width // ncol))
    return (root, right)


def solution(mesh):
    fine = Mesh(mesh.devices.reshape(4, 2, 4, 8), ("x", "core", "y", "z"))
    return jax.shard_map(
        local,
        mesh=fine,
        in_specs=(P(("y", "z"), ("x", "core")), P(("x", "core", "y", "z"), None)),
        out_specs=(P(("x", "core"), ("y", "z")), P(("y", "z"), None)),
        check_vma=False,
    )
```

```python
import functools

import jax
import jax.numpy as jnp
from jax import lax
from jax.experimental import pallas as pl
from jax.experimental.pallas import tpu as pltpu
from jax.sharding import Mesh
from jax.sharding import PartitionSpec as P

ITERS = 8
HIGHEST = lax.Precision.HIGHEST


def shift(value, axis, by):
    size = lax.axis_size(axis)
    return lax.ppermute(value, axis, [(i, (i + by) % size) for i in range(size)])


def high_low(value):
    high = value.astype(jnp.bfloat16)
    return high, (value - high.astype(jnp.float32)).astype(jnp.bfloat16)


def dot3(left, right):
    (lh, ll), (rh, rl) = left, right
    dot = functools.partial(jnp.dot, preferred_element_type=jnp.float32)
    return dot(lh, rh) + (dot(lh, rl) + dot(ll, rh))


WHOLE = pl.BlockSpec(memory_space=pltpu.VMEM)
SCALARS = pl.BlockSpec(memory_space=pltpu.SMEM)


def column(where, offset, depth, count):
    return pl.multiple_of(lax.rem(where + (offset + count), count) * depth, depth)


def first_kernel(offsets, nz, at, q0, q1, q2, q3, own, *rest):
    pieces, (acc, high, low) = rest[:-3], rest[-3:]
    lines = q0.shape[0]
    for k, quarter in enumerate((q0, q1, q2, q3)):
        rows = pl.ds(pl.multiple_of(lax.rem(at[0] + k, 4) * lines, lines), lines)
        high[rows, :], low[rows, :] = high_low(quarter[...])
    depth = own.shape[0]
    cols = pl.ds(column(at[1], 0, depth, nz), depth)
    acc[...] = dot3((high[:, cols], low[:, cols]), high_low(own[...]))
    add_chunks(offsets, nz, at, high, low, pieces, acc)


def add_chunks(offsets, nz, at, high, low, pieces, acc):
    for i, offset in enumerate(offsets):
        chunk = jnp.concatenate([pieces[2 * i][...], pieces[2 * i + 1][...]], axis=0)
        depth = chunk.shape[0]
        cols = pl.ds(column(at[1], offset, depth, nz), depth)
        acc[...] += dot3((high[:, cols], low[:, cols]), high_low(chunk))


def middle_kernel(offsets, nz, at, high, low, before, *rest):
    pieces, acc = rest[:-1], rest[-1]
    acc[...] = before[...]
    add_chunks(offsets, nz, at, high, low, pieces, acc)


def last_kernel(offsets, nz, share, at, high, low, before, *rest):
    pieces, (keep, give, acc) = rest[:-3], rest[-3:]
    acc[...] = before[...]
    add_chunks(offsets, nz, at, high, low, pieces, acc)
    for i in range(keep.shape[0] // share):
        for core, out in ((at[2], keep), (1 - at[2], give)):
            rows = pl.ds(pl.multiple_of((2 * i + core) * share, share), share)
            out[i * share : (i + 1) * share, :] = acc[rows, :]


PARAMS = pltpu.CompilerParams(vmem_limit_bytes=24 << 20)


def cost(flops, size):
    return pl.CostEstimate(flops=flops, bytes_accessed=size, transcendentals=0)


def f32(*shape):
    return jax.ShapeDtypeStruct(shape, jnp.float32)


def bf16(*shape):
    return jax.ShapeDtypeStruct(shape, jnp.bfloat16)


def polar_kernel(at, mine_ref, other_ref, here_ref, there_ref, root_ref, right_ref, mh, ml, mf, xf):
    width = mf.shape[0]
    short, height = root_ref.shape
    chips, tall, _ = mine_ref.shape
    groups, share, _ = here_ref.shape
    for chip in range(chips):
        for core, ref in ((at[1], mine_ref), (1 - at[1], other_ref)):
            rows = pl.ds(pl.multiple_of((2 * chip + core) * tall, tall), tall)
            mf[rows, :] = ref[chip]
    gram = mf[...]
    scale = jnp.sqrt(jnp.sum(gram * gram) + 1e-06)
    root_scale = jnp.sqrt(scale)
    upper = gram / scale
    mf[...] = upper
    mh[...], ml[...] = high_low(upper)
    xf[:short, :] = mf[pl.ds(pl.multiple_of(at[2] * short, short), short), :]
    for group in range(groups):
        for core, ref in ((at[1], here_ref), (1 - at[1], there_ref)):
            row = short + (2 * group + core) * share
            xf[pl.ds(pl.multiple_of(row, share), share), :] = ref[group]

    def advance():
        x = xf[...]
        xf[...] = 1.5 * x - 0.5 * dot3(high_low(x), (mh[...], ml[...]))

    def step(_, carry):
        m = (mh[...], ml[...])
        part = 1.5 * mf[...] - 0.5 * dot3(m, m)
        advance()
        new = 1.5 * part - 0.5 * dot3(high_low(part), m)
        mf[...] = new
        mh[...], ml[...] = high_low(new)
        return carry

    lax.fori_loop(0, ITERS - 1, step, 0)
    advance()
    turned = pltpu.roll(xf[:short, :] * root_scale, lax.rem(width - at[0] * height, width), 1)
    root_ref[...] = turned[:, :height]
    right_ref[...] = xf[short:, :] / root_scale


def polar(at, mine, other, here, there, root):
    width = here.shape[2]
    lines = 2 * here.shape[0] * here.shape[1]
    height, short = root
    half = pltpu.VMEM((width, width), jnp.bfloat16)
    turned, right = pl.pallas_call(
        polar_kernel,
        out_shape=(f32(short, height), f32(lines, width)),
        in_specs=[SCALARS] + [WHOLE] * 4,
        out_specs=(WHOLE, WHOLE),
        scratch_shapes=[
            half,
            half,
            pltpu.VMEM((width, width), jnp.float32),
            pltpu.VMEM((short + lines, width), jnp.float32),
        ],
        compiler_params=PARAMS,
        name="polar",
    )(at, mine, other, here, there)
    return (turned.T, right)


def local(matrix, basis):
    width = basis.shape[1]
    nx, nc, ny, nz = (lax.axis_size(a) for a in ("x", "core", "y", "z"))
    x, c, y, z = (lax.axis_index(a) for a in ("x", "core", "y", "z"))
    depth = basis.shape[0]
    nrow, ncol = nx * nc, ny * nz
    lines = matrix.shape[0]

    span = depth * nz

    def part(k, after=None):
        whole = matrix if after is None else lax.optimization_barrier((matrix, after))[0]
        return lax.dynamic_slice(whole, (0, lax.rem(y + k, ny) * span), (lines, span))

    half = depth // 2
    chunks = {}
    fwd = [basis[:half], basis[half:]]
    bwd = list(fwd)
    quarters = [None] * ny
    for k in range(1, nz // 2 + 1):
        for piece in range(2):
            if k < nz // 2 or piece == 0:
                fwd[piece] = shift(fwd[piece], "z", 1)
            if k < nz // 2 or piece == 1:
                bwd[piece] = shift(bwd[piece], "z", -1)
        if k < nz // 2:
            chunks[-k], chunks[k] = tuple(fwd), tuple(bwd)
        else:
            chunks[k] = (fwd[0], bwd[1])
        if k == 1:
            for j, after in ((1, fwd[0]), (3, bwd[0]), (2, fwd[1])):
                quarters[-j % ny] = shift(part(j, after), "y", j)
        if k == 2:
            quarters[0] = part(0, fwd[0])

    at = jnp.stack([y, z, c]).astype(jnp.int32)
    high = bf16(ny * lines, span)
    total = f32(ny * lines, width)
    each = 6 * ny * lines * depth * width

    def pieces_of(offsets):
        return [piece for k in offsets for piece in chunks[k]]

    offsets = (1, -1, 2, -2)
    acc, high, low = pl.pallas_call(
        functools.partial(first_kernel, offsets, nz),
        out_shape=(total, high, high),
        in_specs=[SCALARS] + [WHOLE] * (5 + 2 * len(offsets)),
        out_specs=(WHOLE,) * 3,
        cost_estimate=cost(5 * each, 8 << 20),
        compiler_params=PARAMS,
        name="first_chunks",
    )(at, *quarters, basis, *pieces_of(offsets))
    offsets = (3, -3)
    acc = pl.pallas_call(
        functools.partial(middle_kernel, offsets, nz),
        out_shape=total,
        in_specs=[SCALARS] + [WHOLE] * (3 + 2 * len(offsets)),
        out_specs=WHOLE,
        cost_estimate=cost(2 * each, 4 << 20),
        compiler_params=PARAMS,
        name="middle_chunks",
    )(at, high, low, acc, *pieces_of(offsets))
    offsets = (4,)
    share = lines // nrow
    keep, give = pl.pallas_call(
        functools.partial(last_kernel, offsets, nz, share),
        out_shape=(f32(ny * lines // nc, width),) * 2,
        in_specs=[SCALARS] + [WHOLE] * (3 + 2 * len(offsets)),
        out_specs=(WHOLE,) * 2,
        scratch_shapes=[pltpu.VMEM((ny * lines, width), jnp.float32)],
        cost_estimate=cost(each, 3 << 20),
        compiler_params=PARAMS,
        name="last_chunk",
    )(at, high, low, acc, *pieces_of(offsets))
    total = (keep + shift(give, "core", 1)).reshape(ny * nx, share, width)
    tiles = lax.all_to_all(total, ("y", "x"), 0, 0, tiled=True)
    own = tiles.sum(axis=0)
    chips = ny * nx
    copies = jnp.broadcast_to(own, (chips, share, width))
    proj = lax.all_to_all(copies, ("y", "x"), 0, 0, tiled=True)
    tall = width // (chips * nc)
    chip = y * nx + x
    flat = proj.reshape(chips * share, width)
    some = lax.dynamic_slice(flat, (0, chip * tall * nc), (chips * share, tall * nc))
    gram = lax.dot_general(some, flat, (((0,), (0,)), ((), ())), precision=HIGHEST)
    keep = lax.dynamic_slice(gram, (c * tall, 0), (tall, width))
    give = lax.dynamic_slice(gram, ((1 - c) * tall, 0), (tall, width))
    gram = keep + shift(give, "core", 1)
    copies = jnp.broadcast_to(gram, (nz, tall, width))
    gram = lax.all_to_all(copies, "z", 0, 0, tiled=True).sum(axis=0)
    copies = jnp.broadcast_to(gram, (chips, tall, width))
    gram = lax.all_to_all(copies, ("y", "x"), 0, 0, tiled=True)
    other = shift(gram, "core", 1)
    here = lax.dynamic_slice(proj, (y * nx, 0, 0), (nx, share, width))
    there = shift(here, "core", 1)
    where = jnp.stack([x * nc + c, c, y * nz + z]).astype(jnp.int32)
    return polar(where, gram, other, here, there, (width // nrow, width // ncol))


def solution(mesh):
    fine = Mesh(mesh.devices.reshape(4, 2, 4, 8), ("x", "core", "y", "z"))
    return jax.shard_map(
        local,
        mesh=fine,
        in_specs=(P(("y", "z"), ("x", "core")), P(("x", "core", "y", "z"), None)),
        out_specs=(P(("x", "core"), ("y", "z")), P(("y", "z"), None)),
        check_vma=False,
    )
```
